32 devices in a mesh: grp: 2 (over y), row: 8 (over z, x), col: 2 (over core).
Axes of the slice: x: 2, y: 2, z: 4, core: 2. Of those that a mesh axis runs over, the one named last changes fastest.
Arguments:
- queries: bfloat16 [1024, 8192], P(('grp', 'row'), 'col'), parts along dimension 0, may hold values from -256 to 256
- key_cache: bfloat16 [512, 512], P(('grp', 'row', 'col')), parts along dimension 0, may hold values from -6 to 6
- value_cache: bfloat16 [512, 512], P(('grp', 'row', 'col')), parts along dimension 0, may hold values from -6 to 6
- tile_active: int32 [8, 2], P('grp'), parts along dimension 0, may hold values from 0 to 1, as said below
- query_step: int32 [1024], P(('grp', 'row')), parts along dimension 0, may hold values from 0 to 63
- key_step: int32 [512], P(('grp', 'row', 'col')), parts along dimension 0, may hold values from 0 to 63, never falling along the last dimension, each value on 1 to 16 neighbouring positions
Outputs:
- attended: bfloat16 [1024, 8192], P(('grp', 'row'), 'col'), parts along dimension 0
The draws below stay inside these ranges and needn't reach their ends.
There are 2 independent parts, one for each index of `grp`. The reference program is written for one: setup_inputs(seed, part) draws one part's arguments, and reference() takes and returns one part's arrays. A program takes and returns all parts, laid end to end along the dimension named above; each array names one. Nothing has to cross between parts.
Inputs may be any that keep to these rules, and one draw needn't show every extreme that they name: `tile_active`: every entry of column 0 is 1. `key_step`: never falls along the cached rows and starts at 0.
All inputs are finite; a program needn't handle non-finite values.
Results may differ from the reference program's by a relative error of at most 0.015.
Values may be sent and summed in bfloat16 or wider, within the bound.
No kernel may reach another device: no remote copies, remote signals or barrier semaphores. Data moves between devices by JAX's collectives and lax.ppermute only.
A program may use at most 64 MiB of HBM per device.

```python
import math
import jax
import jax.numpy as jnp
import numpy as np
from jax import lax

H = 64
KVH = 4
DH = 128
TILE = 128
STEPS = 64
QROWS = 512
KEYS = 256


def cache_values(key):
    source = jax.random.fold_in(key, 11)
    result = jnp.clip(jax.random.normal(source, (KEYS, KVH * DH), jnp.float32), -6.0, 6.0)
    return result


def draw_key_cache(key, part):
    return cache_values(key).astype(jnp.bfloat16)


def draw_queries(key, part):
    noise = jnp.clip(jax.random.normal(jax.random.fold_in(key, 23), (QROWS, H * DH), jnp.float32), -6.0, 6.0)
    return noise.astype(jnp.bfloat16)


def draw_tile_active(key, part):
    tiles_query = QROWS // TILE
    tiles_key = KEYS // TILE
    limits = jax.random.randint(jax.random.fold_in(key, 31), (tiles_query, 1), tiles_key // 4, tiles_key + 1)
    holes = jax.random.randint(jax.random.fold_in(key, 37), (tiles_query, tiles_key), 0, 8)
    positions = jnp.arange(tiles_key, dtype=jnp.int32)[None, :]
    active = (positions < limits) & (holes != 0) | (positions == 0)
    return active.astype(jnp.int32)


def with_ends(entries, own_key, least, top_value):
    index_at = [jax.random.randint(jax.random.fold_in(own_key, axis), (), 0, length) for axis, length in enumerate(entries.shape)]
    longest = entries.shape.index(max(entries.shape))
    next_to = index_at[:longest] + [(index_at[longest] + 1) % entries.shape[longest]] + index_at[longest + 1:]
    return entries.at[tuple(index_at)].set(least).at[tuple(next_to)].set(top_value)


def level_of(own_key, dims, shards, smallest, largest):
    def one(dim, parts):
        steps = jax.random.uniform(jax.random.fold_in(jax.random.fold_in(own_key, 6), dim), (parts,), jnp.float32, smallest / len(shards), largest / len(shards))
        return jnp.repeat(jnp.exp(steps), dims[dim] // parts).reshape((-1,) + (1,) * (len(dims) - dim - 1))

    loudness = one(*shards[0])
    for cut in shards[1:]:
        loudness = loudness * one(*cut)
    return loudness


def profile(count, total, limit, slope):
    portions = [(1 << 20) // math.isqrt(standing ** slope) + 1 for standing in range(2, count + 1)]
    spare, holding = total - limit - (count - 1), [1] * (count - 1)
    while spare > 0:
        movable = [i for i in range(count - 1) if holding[i] < limit]
        whole, left = sum([portions[i] for i in movable]), spare
        for i in movable:
            addition = min(limit - holding[i], max(1, left * portions[i] // whole), spare)
            holding[i] = holding[i] + addition
            spare = spare - addition
    return np.array([limit] + holding)


def ragged(rng, count, total, most, skew):
    if count == 2:
        one = jax.random.randint(rng, (), max(1, total - most), min(most, total - 1) + 1)
        return jnp.stack([one, total - one])
    sizes = jnp.asarray(profile(count, total, most, skew), jnp.int32)
    twos = (count - 1) // 2
    donor, sink = sizes[1:1 + 2 * twos:2], sizes[2:2 + 2 * twos:2]
    room = jnp.minimum(donor - 1, most - sink)
    passed = jax.random.randint(jax.random.fold_in(rng, 1), (twos,), 0, 1 << 20) % (room + 1)
    sizes = sizes.at[1:1 + 2 * twos:2].set(donor - passed).at[2:2 + 2 * twos:2].set(sink + passed)
    return sizes[jax.random.permutation(jax.random.fold_in(rng, 2), count)]


def centred(stream_key, dims, width, limit, split=(), held_as=jnp.bfloat16):
    loudness = level_of(stream_key, dims, split, -0.22, 0.18) if split else 1.0
    entries = jax.random.normal(stream_key, dims, jnp.float32) * width * loudness
    return jnp.minimum(jnp.maximum(entries, -limit), limit).astype(held_as)


def setup_inputs(seed: int = 0, part: int = 0) -> dict:
    streams_of = jax.random.split(jax.random.key(seed), 7)
    part_keys = jax.random.split(jax.random.fold_in(streams_of[6], part), 7)
    queries = draw_queries(jax.random.fold_in(jax.random.fold_in(streams_of[6], part), 71), part)
    key_cache = draw_key_cache(jax.random.fold_in(jax.random.fold_in(streams_of[6], part), 71), part)
    value_cache = centred(part_keys[2], (KEYS, KVH * DH), 1.0, 6.0, ((0, 16),))
    tile_active = draw_tile_active(jax.random.fold_in(jax.random.fold_in(streams_of[6], part), 71), part)
    query_step = with_ends(jax.random.randint(part_keys[4], (QROWS,), 0, STEPS), jax.random.fold_in(part_keys[4], 1), 0, STEPS - 1).astype(jnp.int32)
    key_step = jnp.searchsorted(jnp.cumsum(ragged(part_keys[5], STEPS, KEYS, KEYS // 16, 2)), jnp.arange(KEYS), side="right").astype(jnp.int32)
    return {"queries": queries, "key_cache": key_cache, "value_cache": value_cache, "tile_active": tile_active, "query_step": query_step, "key_step": key_step}


def reference(queries, key_cache, value_cache, tile_active, query_step, key_step):
    groups = H // KVH
    scaling = 1.0 / math.sqrt(DH)
    tile_count = QROWS // TILE
    key_tiles = jnp.arange(KEYS, dtype=jnp.int32) // TILE
    keys_wide = key_cache.astype(jnp.float32).reshape(KEYS, KVH, DH)
    values_wide = value_cache.astype(jnp.float32).reshape(KEYS, KVH, DH)

    def one_tile(inputs):
        query_block, steps_block, tile_row = inputs
        heads = query_block.astype(jnp.float32).reshape(TILE, KVH, groups, DH)
        scores = jnp.einsum('qhgd,khd->hgqk', heads, keys_wide) * scaling
        allowed = (tile_row[key_tiles] == 1)[None, :] & (key_step[None, :] <= steps_block[:, None])
        scores = jnp.where(allowed[None, None], scores, -jnp.inf)
        highest = lax.optimization_barrier(jnp.max(scores, axis=-1, keepdims=True))
        weights = jnp.exp(scores - highest)
        totals = lax.optimization_barrier(jnp.sum(weights, axis=-1))
        rounded = lax.optimization_barrier(weights.astype(jnp.bfloat16)).astype(jnp.float32)
        numerator = jnp.einsum('hgqk,khd->hgqd', rounded, values_wide)
        result = numerator / totals[..., None]
        return result.transpose(2, 0, 1, 3).reshape(TILE, H * DH).astype(jnp.bfloat16)
    blocks = lax.map(one_tile, (queries.reshape(tile_count, TILE, H * DH), query_step.reshape(tile_count, TILE), tile_active))
    return blocks.reshape(QROWS, H * DH)
```

```python
import math

import jax
import jax.numpy as jnp
from jax import lax
from jax.experimental import pallas as pl
from jax.experimental.pallas import tpu as pltpu
from jax.sharding import PartitionSpec as P

H = 64
KVH = 4
DH = 128
TILE = 128
WIDE = 2 * KVH * DH + 128
SCALE = math.log2(math.e) / math.sqrt(DH)
HEADS_PER_STEP = 8


def pack_kernel(keys_ref, values_ref, steps_ref, packed_ref):
    count = keys_ref.shape[0]
    shard = lax.axis_index("row") * lax.axis_size("col") + lax.axis_index("col")
    packed_ref[:, : KVH * DH] = keys_ref[...]
    packed_ref[:, KVH * DH : 2 * KVH * DH] = values_ref[...]
    across = lax.broadcasted_iota(jnp.int32, (count, count), 1)
    down = lax.broadcasted_iota(jnp.int32, (count, count), 0)
    steps = jnp.where(across == down, steps_ref[...].reshape(1, count), 0)
    steps = jnp.sum(steps.astype(jnp.float32), axis=1, keepdims=True)
    lane = lax.broadcasted_iota(jnp.int32, (count, 128), 1)
    position = shard * count + lax.broadcasted_iota(jnp.int32, (count, 128), 0)
    tile = (position // TILE).astype(jnp.float32)
    marks = jnp.where(lane == 0, steps, jnp.where(lane == 1, tile, 0.0))
    packed_ref[:, 2 * KVH * DH :] = marks.astype(jnp.bfloat16)


def pack(key_cache, value_cache, key_step):
    return pl.pallas_call(
        pack_kernel,
        out_shape=jax.ShapeDtypeStruct((key_cache.shape[0], WIDE), jnp.bfloat16),
        name="pack",
    )(key_cache, value_cache, key_step)


def attend_kernel(active_ref, queries_ref, steps_ref, *refs, piece_rows, local_heads):
    pieces = refs[: len(piece_rows)]
    out_ref, keys_ref, values_ref, bias_ref = refs[len(piece_rows) :]
    key_count = sum(piece_rows)
    query_count = queries_ref.shape[0]
    step = pl.program_id(0)
    groups = H // KVH
    contract_last = (((1,), (1,)), ((), ()))

    @pl.when(step == 0)
    def prepare():
        first = lax.axis_index("col") * local_heads
        start = 0
        marks = []
        for ref, rows in zip(pieces, piece_rows):
            for head in range(local_heads):
                key_lane = pl.multiple_of((first + head) * DH, DH)
                value_lane = pl.multiple_of((KVH + first + head) * DH, DH)
                keys_ref[head, start : start + rows, :] = ref[:, pl.ds(key_lane, DH)]
                values_ref[head, start : start + rows, :DH] = ref[:, pl.ds(value_lane, DH)]
            marks.append(ref[:, 2 * KVH * DH :])
            start += rows
        values_ref[:, :, DH:] = jnp.ones((local_heads, key_count, DH), jnp.bfloat16)
        marks = jnp.concatenate(marks, axis=0)
        pick = lax.broadcasted_iota(jnp.int32, (8, 128), 0) == lax.broadcasted_iota(
            jnp.int32, (8, 128), 1
        )
        rows = lax.dot_general(
            pick.astype(jnp.bfloat16), marks, contract_last, preferred_element_type=jnp.float32
        )
        key_steps, key_tiles = rows[0:1, :], rows[1:2, :]
        across = lax.broadcasted_iota(jnp.int32, (query_count, query_count), 1)
        down = lax.broadcasted_iota(jnp.int32, (query_count, query_count), 0)
        query_steps = jnp.where(across == down, steps_ref[...].reshape(1, query_count), 0)
        query_steps = jnp.sum(query_steps.astype(jnp.float32), axis=1, keepdims=True)
        block = math.gcd(query_count, TILE)
        for at in range(0, query_count, block):
            tile = (lax.axis_index("row") * query_count + at) // TILE
            active = jnp.zeros_like(key_steps)
            for key_tile in range(active_ref.shape[1]):
                listed = (active_ref[tile, key_tile] == 1).astype(jnp.float32)
                active = jnp.where(key_tiles == float(key_tile), listed, active)
            marked = jnp.where(active > 0.5, key_steps, 1e9)
            allowed = marked <= query_steps[at : at + block]
            bias_ref[at : at + block, :] = jnp.where(allowed, 0.0, -1e30)

    head = step // (groups // HEADS_PER_STEP)
    keys = keys_ref[head]
    values = values_ref[head]
    bias = bias_ref[...]
    for index in range(HEADS_PER_STEP):
        lanes = slice(index * DH, (index + 1) * DH)
        scores = lax.dot_general(
            queries_ref[:, lanes], keys, contract_last, preferred_element_type=jnp.float32
        )
        scores = scores + bias
        highest = jnp.max(scores, axis=1, keepdims=True)
        weights = jnp.exp2((scores - highest) * SCALE).astype(jnp.bfloat16)
        sums = jnp.dot(weights, values, preferred_element_type=jnp.float32)
        out_ref[:, lanes] = (sums[:, :DH] / sums[:, DH:]).astype(jnp.bfloat16)


def attend(pieces, queries, tile_active, query_step, local_heads):
    query_count, width = queries.shape
    piece_rows = tuple(piece.shape[0] for piece in pieces)
    key_count = sum(piece_rows)
    lanes = HEADS_PER_STEP * DH

    def whole(shape):
        return pl.BlockSpec(shape, lambda step: (0,) * len(shape))

    def kernel(*refs):
        attend_kernel(*refs, piece_rows=piece_rows, local_heads=local_heads)

    return pl.pallas_call(
        kernel,
        grid=(width // lanes,),
        in_specs=[
            pl.BlockSpec(memory_space=pltpu.SMEM),
            pl.BlockSpec((query_count, lanes), lambda step: (0, step)),
            whole(query_step.shape),
            *[whole(piece.shape) for piece in pieces],
        ],
        out_specs=pl.BlockSpec((query_count, lanes), lambda step: (0, step)),
        out_shape=jax.ShapeDtypeStruct(queries.shape, jnp.bfloat16),
        scratch_shapes=[
            pltpu.VMEM((local_heads, key_count, DH), jnp.bfloat16),
            pltpu.VMEM((local_heads, key_count, 2 * DH), jnp.bfloat16),
            pltpu.VMEM((query_count, key_count), jnp.float32),
        ],
        name="attend",
    )(tile_active, queries, query_step, *pieces)


def exchange(packed):
    rows, columns = lax.axis_size("row"), lax.axis_size("col")

    def swap(array):
        return lax.ppermute(array, "col", [(0, 1), (1, 0)])

    def send(array, first, second):
        moves = [(row * 2 + col, (row ^ (first, second)[col]) * 2 + col) for row in range(rows) for col in range(2)]
        return lax.ppermute(array, ("row", "col"), moves)

    if columns != 2 or rows != 8:
        return [lax.all_gather(packed, ("row", "col"), axis=0, tiled=True)]
    other = swap(packed)
    pair = jnp.concatenate([packed, other], axis=0)
    received = [send(packed, 7, 7)] + [send(pair, a, b) for a, b in ((6, 5), (4, 3), (2, 1))]
    return [packed, other] + received + [swap(array) for array in received]


def per_device(queries, key_cache, value_cache, tile_active, query_step, key_step):
    local_heads = KVH // lax.axis_size("col")
    packed = pack(key_cache, value_cache, key_step)
    return attend(exchange(packed), queries, tile_active, query_step, local_heads)


def solution(mesh):
    in_specs = (
        P(("grp", "row"), "col"),
        P(("grp", "row", "col"), None),
        P(("grp", "row", "col"), None),
        P("grp", None),
        P(("grp", "row")),
        P(("grp", "row", "col")),
    )
    out_specs = P(("grp", "row"), "col")
    return jax.shard_map(
        per_device, mesh=mesh, in_specs=in_specs, out_specs=out_specs, check_vma=False
    )
```
